256 devices in a mesh: grp: 4 (over z_hi, core), dev: 64 (over x, z_lo, y).
Axes of the slice: x: 4, y: 4, z: 8 (z_hi: 2, z_lo: 4; z = z_hi * 4 + z_lo), core: 2. Of those that a mesh axis runs over, the one named last changes fastest.
Arguments:
- tables: float32 [4, 524288, 128], P(None, ('grp', 'dev')), may hold values from -6 to 6
- accum: float32 [4, 524288], P(None, ('grp', 'dev')), may hold values from 0.01 to 10
- block_position: int32 [4, 4096], replicated, may hold values from 0 to 4095, as said below
- lookup_ids: int32 [65536, 4], P(('grp', 'dev')), may hold values from 0 to 524287, as said below
Outputs:
- new_tables: float32 [4, 524288, 128], P('grp', 'dev')
- new_accum: float32 [4, 524288], P('grp', 'dev')
- looked: float32 [65536, 4, 128], P(('grp', 'dev'))
The draws below stay inside these ranges and needn't reach their ends.
Inputs may be any that keep to these rules, and one draw needn't show every extreme that they name: `block_position`: for each table a permutation of 0 to 4095. Old block b lies on the device b // 16 of grp+dev; call its dev index its source, and p // 64 the owner of new block p. For every table, source and owner, at most 2 blocks of that source go to that owner, and 2 is reached. `lookup_ids`: the owner of an id of table t is block_position[t, id // 128] // 64. Among one device's 256 rows, at most 8 ids of one table have one owner, and 8 is reached for every device and table.
All inputs are finite; a program needn't handle non-finite values.
Results may differ from the reference program's by a relative error of at most 0.00002.
Values sent between devices are 32-bit elements; how exact they have to be, the bound alone decides.
No kernel may reach another device: no remote copies, remote signals or barrier semaphores. Data moves between devices by JAX's collectives and lax.ppermute only.
A program may use at most 128 MiB of HBM per device.

```python
import math
import jax
import jax.numpy as jnp

DIM = 128
TILE = 128
BLK_DEV = 64
LOOK_DEV = 256
TABLES = 4
ROWS = 524288
N_GRP = 4
N_DEV = 64


def band_counts(key_first, key_second, length):
    starts = jax.random.permutation(key_first, N_DEV)
    shifts = jax.random.permutation(key_second, N_DEV)
    offset = (shifts[None, :] - starts[:, None]) % N_DEV
    return jnp.maximum((length - 1 - offset) // N_DEV + 1, 0).astype(jnp.int32)


def positions_table(table_key):
    keys = jax.random.split(table_key, 6)
    longer = BLK_DEV // 2 + 1
    counts = band_counts(keys[0], keys[1], longer) + band_counts(keys[2], keys[3], BLK_DEV - longer)
    owners = jnp.arange(N_DEV, dtype=jnp.int32)
    targets = jax.vmap(lambda count: jnp.repeat(owners, count, total_repeat_length=BLK_DEV))(counts)
    source_keys = jax.random.split(keys[4], N_DEV)
    shuffled = jax.vmap(lambda one_key, line: jax.random.permutation(one_key, line))(source_keys, targets)
    flat = shuffled.reshape(-1).astype(jnp.int32)
    total = N_DEV * BLK_DEV
    breaker = jax.random.permutation(keys[5], total).astype(jnp.int32)
    ordering = jnp.argsort(flat * total + breaker, stable=True)
    placed = jnp.zeros((total,), jnp.int32).at[ordering].set(jnp.arange(total, dtype=jnp.int32))
    per_old = placed.reshape(N_DEV, N_GRP, BLK_DEV // N_GRP).transpose(1, 0, 2)
    return per_old.reshape(-1)


def make_positions(key):
    base = jax.random.fold_in(key, 11)
    table_keys = jax.vmap(lambda number: jax.random.fold_in(base, number))(jnp.arange(N_GRP))
    return jax.vmap(positions_table)(table_keys)


def draw_block_position(key, part):
    return make_positions(key).astype(jnp.int32)


def draw_lookup_ids(key, part):
    positions = make_positions(key)
    inverse = jnp.argsort(positions, axis=1).astype(jnp.int32)
    base = jax.random.fold_in(key, 23)
    limit = 2 * LOOK_DEV // N_DEV

    def one_block(device, table):
        block_key = jax.random.fold_in(jax.random.fold_in(base, device), table)
        keys = jax.random.split(block_key, 5)
        chosen = jax.random.randint(keys[0], (), 0, N_DEV)
        others = jax.random.permutation(keys[1], (N_DEV - 1) * limit)[:LOOK_DEV - limit] // limit
        others = others + (others >= chosen).astype(others.dtype)
        owner_list = jnp.concatenate([jnp.full((limit,), chosen, jnp.int32), others.astype(jnp.int32)])
        owner_list = jax.random.permutation(keys[2], owner_list)
        within = jax.random.randint(keys[3], (LOOK_DEV,), 0, BLK_DEV)
        offset = jax.random.randint(keys[4], (LOOK_DEV,), 0, TILE)
        inverse_row = inverse[table]
        return inverse_row[owner_list * BLK_DEV + within] * TILE + offset
    devices = jnp.arange(N_GRP * N_DEV)
    tables_list = jnp.arange(N_GRP)
    drawn = jax.vmap(lambda device: jax.vmap(lambda table: one_block(device, table))(tables_list))(devices)
    return drawn.transpose(0, 2, 1).reshape(N_GRP * N_DEV * LOOK_DEV, N_GRP).astype(jnp.int32)


def level_of(key, extent, cuts, smallest, largest):
    gain, own = 1.0, jax.random.fold_in(key, 6)
    for axis_at, parts in cuts:
        steps = jnp.exp(jax.random.uniform(jax.random.fold_in(own, axis_at), (parts,), jnp.float32, smallest / len(cuts), largest / len(cuts)))
        gain = gain * jnp.repeat(steps, extent[axis_at] // parts).reshape([-1 if axis == axis_at else 1 for axis in range(len(extent))])
    return gain


def scatter_about(key, shape, scale, most, cuts=(), held_as=jnp.bfloat16):
    values = jax.random.normal(key, shape, jnp.float32) * scale
    if len(cuts) > 0:
        values = level_of(key, shape, cuts, -0.22, 0.18) * values
    return jnp.clip(values, min=-most, max=most).astype(held_as)


def setup_inputs(seed: int = 0) -> dict:
    key_list = jax.random.split(jax.random.key(seed), 5)
    tables = scatter_about(key_list[0], (TABLES, ROWS, DIM), 1.0, 6.0, ((1, 256),), jnp.float32)
    accum = jnp.clip(jnp.exp(math.log(10.0) - 6.9077553 * jax.random.uniform(key_list[1], (TABLES, ROWS), jnp.float32) ** level_of(key_list[1], (TABLES, ROWS), ((1, 256),), -0.2, 0.2)), 0.01, 10.0)
    block_position = draw_block_position(jax.random.fold_in(key_list[4], 71), 0)
    lookup_ids = draw_lookup_ids(jax.random.fold_in(key_list[4], 71), 0)
    return dict(tables=tables, accum=accum, block_position=block_position, lookup_ids=lookup_ids)


def reference(tables, accum, block_position, lookup_ids):
    table_count, row_count, width = tables.shape
    block_count = block_position.shape[1]
    tile_rows = row_count // block_count
    inverse = jnp.argsort(block_position, axis=1).astype(jnp.int32)
    blocks = tables.reshape(table_count, block_count, tile_rows, width)
    moved = jnp.take_along_axis(blocks, inverse[:, :, None, None], axis=1)
    new_tables = moved.reshape(table_count, row_count, width)
    sums = accum.reshape(table_count, block_count, tile_rows)
    new_accum = jnp.take_along_axis(sums, inverse[:, :, None], axis=1).reshape(table_count, row_count)
    which = jnp.arange(table_count, dtype=jnp.int32)[None, :]
    looked = tables[which, lookup_ids]
    return new_tables, new_accum, looked
```

```python
import jax
import jax.numpy as jnp
from jax import lax
from jax.experimental import pallas as pl
from jax.experimental.pallas import tpu as pltpu
from jax.sharding import PartitionSpec as P

TILE = 128


def spread_rows(tables, parts):
    count, rows, width = tables.shape
    blocks = rows // TILE
    piece = TILE // parts

    def kernel(in_ref, out_ref):
        def one(block, carry):
            for part in range(parts):
                out_ref[part, block] = in_ref[0, pl.ds(block * TILE + part * piece, piece), :]
            return carry

        lax.fori_loop(0, blocks, one, 0)

    return pl.pallas_call(
        kernel,
        grid=(count,),
        in_specs=[pl.BlockSpec((1, rows, width), lambda t: (t, 0, 0))],
        out_specs=pl.BlockSpec((parts, blocks, piece, width), lambda t: (t, 0, 0, 0)),
        out_shape=jax.ShapeDtypeStruct((count * parts, blocks, piece, width), tables.dtype),
        name="spread_rows",
    )(tables)


def place_pieces(pieces, slots, sums, notes, total):
    count, piece, width = pieces.shape
    owners = sums.shape[0]
    per_owner = total // owners
    chunk = 512
    batch = 16

    def kernel(slots_ref, in_ref, sums_ref, notes_ref, out_ref):
        step = pl.program_id(0)

        @pl.when(step == 0)
        def _():
            for owner in range(owners):
                out_ref[owner * per_owner + per_owner - 2] = sums_ref[owner]
                out_ref[owner * per_owner + per_owner - 1] = notes_ref[owner]

        def some(at, carry):
            first = at * batch
            held = [in_ref[first + k] for k in range(batch)]
            for k in range(batch):
                out_ref[slots_ref[step * chunk + first + k]] = held[k]
            return carry

        lax.fori_loop(0, chunk // batch, some, 0)

    return pl.pallas_call(
        kernel,
        grid_spec=pltpu.PrefetchScalarGridSpec(
            num_scalar_prefetch=1,
            grid=(count // chunk,),
            in_specs=[
                pl.BlockSpec((chunk, piece, width), lambda c, s: (c, 0, 0)),
                pl.BlockSpec((owners, piece, width), lambda c, s: (0, 0, 0)),
                pl.BlockSpec((owners, piece, width), lambda c, s: (0, 0, 0)),
            ],
            out_specs=pl.BlockSpec((total, piece, width), lambda c, s: (0, 0, 0)),
        ),
        out_shape=jax.ShapeDtypeStruct((total, piece, width), pieces.dtype),
        name="place_pieces",
    )(slots, pieces, sums, notes)


def pick_rows(rows, which):
    count = which.shape[0]
    width = rows.shape[2]
    batch = 16

    def kernel(which_ref, in_ref, out_ref):
        def some(at, carry):
            first = at * batch
            held = [in_ref[which_ref[first + k]] for k in range(batch)]
            for k in range(batch):
                out_ref[first + k] = held[k]
            return carry

        lax.fori_loop(0, count // batch, some, 0)

    return pl.pallas_call(
        kernel,
        grid_spec=pltpu.PrefetchScalarGridSpec(
            num_scalar_prefetch=1,
            grid=(1,),
            in_specs=[pl.BlockSpec(rows.shape, lambda c, w: (0, 0, 0))],
            out_specs=pl.BlockSpec((count, 1, width), lambda c, w: (0, 0, 0)),
        ),
        out_shape=jax.ShapeDtypeStruct((count, 1, width), rows.dtype),
        name="pick_rows",
    )(which, rows)


def join_rows(got, blocks):
    parts, _, piece, width = got.shape
    chunk = 8

    def kernel(in_ref, out_ref):
        first = pl.program_id(0) * chunk

        def one(block, carry):
            for part in range(parts):
                out_ref[block * parts + part] = in_ref[part, first + block]
            return carry

        lax.fori_loop(0, chunk, one, 0)

    return pl.pallas_call(
        kernel,
        grid=(blocks // chunk,),
        in_specs=[pl.BlockSpec(got.shape, lambda c: (0, 0, 0, 0))],
        out_specs=pl.BlockSpec((chunk * parts, piece, width), lambda c: (c, 0, 0)),
        out_shape=jax.ShapeDtypeStruct((blocks * parts, piece, width), got.dtype),
        name="join_rows",
    )(got)


def swap_groups(parts, axis):
    peers = lax.axis_size(axis)
    me = lax.axis_index(axis)
    held = [lax.dynamic_index_in_dim(parts, me, 0, keepdims=False)]
    for by in range(1, peers):
        part = lax.dynamic_index_in_dim(parts, (me + by) % peers, 0, keepdims=False)
        held.append(lax.ppermute(part, axis, [(i, (i + by) % peers) for i in range(peers)]))
    return jnp.stack(held)[(me - jnp.arange(peers)) % peers]


def body(tables, accum, block_position, lookup_ids):
    groups = lax.axis_size("grp")
    shards = lax.axis_size("dev")
    my_group = lax.axis_index("grp")
    my_shard = lax.axis_index("dev")
    both = ("grp", "dev")
    table_count, old_rows, width = tables.shape
    per_old = old_rows // TILE
    local = groups * per_old
    piece = TILE // shards
    look_rows = lookup_ids.shape[0]
    limit = 2 * look_rows // shards

    spread = spread_rows(tables, shards)
    spread, accum, block_position, lookup_ids = lax.optimization_barrier(
        (spread, accum, block_position, lookup_ids)
    )
    pieces = lax.all_to_all(spread, both, split_axis=0, concat_axis=0, tiled=True)

    table_ids = jnp.arange(table_count, dtype=jnp.int32)[None, :]
    id_place = block_position[table_ids, lookup_ids // TILE]
    owner = id_place // local
    local_row = id_place % local * TILE + lookup_ids % TILE
    owner_marks = (owner[..., None] == jnp.arange(shards, dtype=jnp.int32)[None, None, :]).astype(jnp.int32)
    owner_order = jnp.sum((jnp.cumsum(owner_marks, axis=0) - owner_marks) * owner_marks, axis=2)
    table_grid = jnp.broadcast_to(table_ids, owner.shape)
    asking = (
        jnp.full((table_count, shards, limit), -1, jnp.int32)
        .at[table_grid, owner, owner_order]
        .set(local_row)
    )

    small = jnp.concatenate(
        [
            accum.reshape(table_count, per_old, TILE),
            asking.astype(jnp.float32).reshape(table_count, -1, TILE),
        ],
        axis=1,
    )
    small = swap_groups(small, "grp")
    block_sums = small[:, :per_old].reshape(local, TILE)
    passed = small[:, per_old:].reshape(groups, shards, limit)

    counter = jnp.arange(local, dtype=jnp.int32)
    old_index = (counter // per_old * shards + my_shard) * per_old + counter % per_old
    position_row = lax.dynamic_index_in_dim(block_position, my_group, 0, keepdims=False)
    new_place = position_row[old_index]
    target = new_place // local
    slot_place = new_place % local
    longer = local // 2 + 1
    capacity = -(-longer // shards) + -(-(local - longer) // shards)
    marks = (target[:, None] == jnp.arange(shards, dtype=jnp.int32)[None, :]).astype(jnp.int32)
    order_in = jnp.sum((jnp.cumsum(marks, axis=0) - marks) * marks, axis=1)
    slot_index = target * capacity + order_in
    source_of = jnp.zeros((shards * capacity,), jnp.int32).at[slot_index].set(counter)
    filled = jnp.zeros((shards * capacity,), jnp.int32).at[slot_index].set(1)
    send_sums = block_sums[source_of].reshape(shards, capacity, TILE)
    send_place = jnp.where(filled == 1, slot_place[source_of], -1).reshape(shards, capacity)
    notes = jnp.concatenate(
        [send_place.astype(jnp.float32), passed.transpose(1, 0, 2).reshape(shards, groups * limit)], axis=1
    )
    notes = jnp.pad(notes[:, None, :], ((0, 0), (0, piece - 1), (0, TILE - notes.shape[1])))

    per_owner = local + 2
    slots = position_row + position_row // local * 2
    sending = place_pieces(
        pieces.reshape(-1, piece, width), slots, send_sums, notes, shards * per_owner
    ).reshape(shards, per_owner, piece, width)
    got = lax.all_to_all(sending, "dev", split_axis=0, concat_axis=0, tiled=True)

    got_notes = got[:, local + 1, 0, : capacity + groups * limit].astype(jnp.int32)
    wanted = got_notes[:, capacity:].reshape(shards, groups, limit).transpose(1, 0, 2).reshape(-1)
    wanted = jnp.maximum(wanted, 0)
    inside = wanted % TILE
    at_row = (inside // piece * per_owner + wanted // TILE) * piece + inside % piece
    answer = pick_rows(got.reshape(-1, 1, width), at_row).reshape(groups * shards, limit, width)
    returned = lax.all_to_all(answer, both, split_axis=0, concat_axis=0, tiled=True)

    new_table = join_rows(got, local).reshape(1, local * TILE, width)
    flat_place = got_notes[:, :capacity].reshape(-1)
    landing = jnp.where(flat_place >= 0, flat_place, local)
    picker = (
        jnp.zeros((local,), jnp.int32)
        .at[landing]
        .set(jnp.arange(shards * capacity, dtype=jnp.int32), mode="drop")
    )
    got_sums = got[:, local].reshape(shards * capacity, TILE)
    new_accum = got_sums[picker].reshape(1, local * TILE)

    slot = ((table_grid * shards + owner) * limit + owner_order).reshape(-1)
    looked = pick_rows(returned.reshape(-1, 1, width), slot).reshape(look_rows, table_count, width)
    return (new_table, new_accum, looked)


def solution(mesh):
    placed = (P(None, ("grp", "dev"), None), P(None, ("grp", "dev")), P(), P(("grp", "dev"), None))
    return jax.shard_map(
        body,
        mesh=mesh,
        in_specs=placed,
        out_specs=(P("grp", "dev", None), P("grp", "dev"), P(("grp", "dev"), None, None)),
        check_vma=False,
    )
```

```python
import jax
import jax.numpy as jnp
from jax import lax
from jax.experimental import pallas as pl
from jax.experimental.pallas import tpu as pltpu
from jax.sharding import PartitionSpec as P

TILE = 128


VMEM = pl.BlockSpec(memory_space=pltpu.VMEM)
SMEM = pl.BlockSpec(memory_space=pltpu.SMEM)
HBM = pl.BlockSpec(memory_space=pltpu.HBM)
ROOM = pltpu.CompilerParams(vmem_limit_bytes=16 * 2**20)


def spread_rows(tables, parts):
    count, rows, width = tables.shape
    blocks = rows // TILE
    piece = TILE // parts
    shape = (count * parts, blocks, piece, width)

    def kernel(in_ref, out_ref, held, came, left):
        def fetch(table):
            return pltpu.make_async_copy(in_ref.at[table], held.at[table], came.at[table])

        def table_out(table):
            return out_ref.at[pl.ds(table * parts, parts)]

        for table in range(count):
            fetch(table).start()
        for table in range(count):
            fetch(table).wait()
            for block in range(blocks):
                pltpu.make_async_copy(held.at[table, block], table_out(table).at[:, block], left.at[table]).start()
        for table in range(count):
            pltpu.make_async_copy(table_out(table), table_out(table), left.at[table]).wait()

    return pl.pallas_call(
        kernel,
        in_specs=[HBM],
        out_specs=HBM,
        out_shape=jax.ShapeDtypeStruct(shape, tables.dtype),
        scratch_shapes=[
            pltpu.VMEM((count, blocks, parts, piece, width), tables.dtype),
            pltpu.SemaphoreType.DMA((count,)),
            pltpu.SemaphoreType.DMA((count,)),
        ],
        name="spread_rows",
    )(tables.reshape(count, blocks, parts, piece, width))


def place_pieces(pieces, slots, sums, notes, total):
    count, piece, width = pieces.shape
    owners = sums.shape[0]
    per_owner = total // owners
    chunk = 512
    steps = count // chunk
    batch = 64

    def kernel(slots_ref, in_ref, sums_ref, notes_ref, out_ref, held, places, came, told):
        def fetch(step):
            span = pl.ds(step * chunk, chunk)
            return pltpu.make_async_copy(in_ref.at[span], held.at[span], came.at[step])

        listing = pltpu.make_async_copy(slots_ref, places, told)
        listing.start()
        for step in range(steps):
            fetch(step).start()
        for owner in range(owners):
            out_ref[owner * per_owner + per_owner - 2] = sums_ref[owner]
            out_ref[owner * per_owner + per_owner - 1] = notes_ref[owner]
        listing.wait()

        def one(step, carry):
            fetch(step).wait()

            def some(at, carry):
                first = step * chunk + at * batch
                rows = [held[first + k] for k in range(batch)]
                for k in range(batch):
                    out_ref[places[first + k]] = rows[k]
                return carry

            return lax.fori_loop(0, chunk // batch, some, carry)

        lax.fori_loop(0, steps, one, 0)

    return pl.pallas_call(
        kernel,
        in_specs=[HBM, HBM, VMEM, VMEM],
        out_specs=VMEM,
        out_shape=jax.ShapeDtypeStruct((total, piece, width), pieces.dtype),
        scratch_shapes=[
            pltpu.VMEM((count, piece, width), pieces.dtype),
            pltpu.SMEM((count,), jnp.int32),
            pltpu.SemaphoreType.DMA((steps,)),
            pltpu.SemaphoreType.DMA,
        ],
        compiler_params=ROOM,
        name="place_pieces",
    )(slots, pieces, sums, notes)


def pick_loop(which_ref, in_ref, out_ref, spots, stride):
    batch = 32

    def one(line, carry):
        for first in range(0, len(spots), batch):
            rows = [in_ref[which_ref[line, k]] for k in range(first, first + batch)]
            for k in range(batch):
                out_ref[line * stride + spots[first + k]] = rows[k]
        return carry

    lax.fori_loop(0, which_ref.shape[0], one, 0)


def pick_rows(rows, which):
    lines, lanes = which.shape
    width = rows.shape[2]

    def kernel(which_ref, in_ref, out_ref):
        pick_loop(which_ref, in_ref, out_ref, range(lanes), lanes)

    return pl.pallas_call(
        kernel,
        in_specs=[SMEM, VMEM],
        out_specs=VMEM,
        out_shape=jax.ShapeDtypeStruct((lines * lanes, 1, width), rows.dtype),
        compiler_params=ROOM,
        name="pick_rows",
    )(which, rows)


def answer_and_join(got, which, blocks, spots, stride):
    parts, _, piece, width = got.shape

    def kernel(which_ref, rows_ref, got_ref, out_ref, table_ref, sums_ref, left):
        for part in range(parts):
            pltpu.make_async_copy(got_ref.at[part, pl.ds(0, blocks)], table_ref.at[:, part], left).start()
        for part in range(parts):
            sums_ref[part] = got_ref[part, blocks]
        pick_loop(which_ref, rows_ref, out_ref, spots, stride)
        pltpu.make_async_copy(table_ref, table_ref, left).wait()

    return pl.pallas_call(
        kernel,
        in_specs=[SMEM, VMEM, VMEM],
        out_specs=(VMEM, HBM, VMEM),
        out_shape=(
            jax.ShapeDtypeStruct((parts * len(spots), 1, width), got.dtype),
            jax.ShapeDtypeStruct((blocks, parts, piece, width), got.dtype),
            jax.ShapeDtypeStruct((parts, piece, width), got.dtype),
        ),
        scratch_shapes=[pltpu.SemaphoreType.DMA],
        compiler_params=ROOM,
        name="answer_and_join",
    )(which, got.reshape(-1, 1, width), got)


def swap_groups(parts, axis):
    peers = lax.axis_size(axis)
    me = lax.axis_index(axis)
    held = [lax.dynamic_index_in_dim(parts, me, 0, keepdims=False)]
    for by in range(1, peers):
        part = lax.dynamic_index_in_dim(parts, (me + by) % peers, 0, keepdims=False)
        held.append(lax.ppermute(part, axis, [(i, (i + by) % peers) for i in range(peers)]))
    return jnp.stack(held)[(me - jnp.arange(peers)) % peers]


def body(tables, accum, block_position, lookup_ids):
    groups = lax.axis_size("grp")
    shards = lax.axis_size("dev")
    my_group = lax.axis_index("grp")
    my_shard = lax.axis_index("dev")
    both = ("grp", "dev")
    table_count, old_rows, width = tables.shape
    per_old = old_rows // TILE
    local = groups * per_old
    piece = TILE // shards
    look_rows = lookup_ids.shape[0]
    limit = 2 * look_rows // shards

    spread = spread_rows(tables, shards)
    spread, accum, block_position, lookup_ids = lax.optimization_barrier(
        (spread, accum, block_position, lookup_ids)
    )
    pieces = lax.all_to_all(spread, both, split_axis=0, concat_axis=0, tiled=True)

    table_ids = jnp.arange(table_count, dtype=jnp.int32)[None, :]
    id_place = block_position[table_ids, lookup_ids // TILE]
    owner = id_place // local
    per_owner = local + 2
    inside = lookup_ids % TILE
    at_row = (inside // piece * per_owner + id_place % local) * piece + inside % piece
    owner_marks = (owner[..., None] == jnp.arange(shards, dtype=jnp.int32)[None, None, :]).astype(jnp.int32)
    owner_order = jnp.sum((jnp.cumsum(owner_marks, axis=0) - owner_marks) * owner_marks, axis=2)
    table_grid = jnp.broadcast_to(table_ids, owner.shape)
    asking = (
        jnp.zeros((table_count, shards, limit), jnp.int32)
        .at[table_grid, owner, owner_order]
        .set(at_row)
    )

    slot = ((table_grid * shards + owner) * limit + owner_order).reshape(-1, TILE)

    small = jnp.concatenate(
        [
            accum.reshape(table_count, per_old, TILE),
            asking.astype(jnp.float32).reshape(table_count, -1, TILE),
        ],
        axis=1,
    )
    small = swap_groups(small, "grp")
    block_sums = small[:, :per_old].reshape(local, TILE)
    passed = small[:, per_old:].reshape(groups, shards, limit)

    counter = jnp.arange(local, dtype=jnp.int32)
    old_index = (counter // per_old * shards + my_shard) * per_old + counter % per_old
    position_row = lax.dynamic_index_in_dim(block_position, my_group, 0, keepdims=False)
    new_place = position_row[old_index]
    target = new_place // local
    slot_place = new_place % local
    longer = local // 2 + 1
    capacity = -(-longer // shards) + -(-(local - longer) // shards)
    marks = (target[:, None] == jnp.arange(shards, dtype=jnp.int32)[None, :]).astype(jnp.int32)
    order_in = jnp.sum((jnp.cumsum(marks, axis=0) - marks) * marks, axis=1)
    slot_index = target * capacity + order_in
    source_of = jnp.zeros((shards * capacity,), jnp.int32).at[slot_index].set(counter)
    filled = jnp.zeros((shards * capacity,), jnp.int32).at[slot_index].set(1)
    send_sums = block_sums[source_of].reshape(shards, capacity, TILE)
    send_place = jnp.where(filled == 1, slot_place[source_of], -1).reshape(shards, capacity)
    notes = jnp.concatenate(
        [passed.transpose(1, 0, 2).reshape(shards, groups * limit), send_place.astype(jnp.float32)], axis=1
    )
    notes = jnp.pad(notes[:, None, :], ((0, 0), (0, piece - 1), (0, TILE - notes.shape[1])))

    pieces, slot = lax.optimization_barrier((pieces, slot))

    slots = position_row + position_row // local * 2
    sending = place_pieces(
        pieces.reshape(-1, piece, width), slots, send_sums, notes, shards * per_owner
    ).reshape(shards, per_owner, piece, width)
    got = lax.all_to_all(sending, "dev", split_axis=0, concat_axis=0, tiled=True)

    asked = groups * limit
    got_notes = got[:, local + 1, 0].astype(jnp.int32)
    spots = [(k // limit * shards) * limit + k % limit for k in range(asked)]
    answer, new_table, got_sums = answer_and_join(got, got_notes, local, spots, limit)
    answer = answer.reshape(groups * shards, limit, width)
    returned = lax.all_to_all(answer, both, split_axis=0, concat_axis=0, tiled=True)

    new_table = new_table.reshape(1, local * TILE, width)
    got_sums, late_notes = lax.optimization_barrier((got_sums, got_notes))
    flat_place = late_notes[:, asked : asked + capacity].reshape(-1)
    landing = jnp.where(flat_place >= 0, flat_place, local)
    picker = (
        jnp.zeros((local,), jnp.int32)
        .at[landing]
        .set(jnp.arange(shards * capacity, dtype=jnp.int32), mode="drop")
    )
    new_accum = got_sums.reshape(shards * capacity, TILE)[picker].reshape(1, local * TILE)

    looked = pick_rows(returned.reshape(-1, 1, width), slot)
    looked = looked.reshape(look_rows, table_count, width)
    return (new_table, new_accum, looked)


def solution(mesh):
    placed = (P(None, ("grp", "dev"), None), P(None, ("grp", "dev")), P(), P(("grp", "dev"), None))
    return jax.shard_map(
        body,
        mesh=mesh,
        in_specs=placed,
        out_specs=(P("grp", "dev", None), P("grp", "dev"), P(("grp", "dev"), None, None)),
        check_vma=False,
    )
```

```python
import jax
import jax.numpy as jnp
from jax import lax
from jax.experimental import pallas as pl
from jax.experimental.pallas import tpu as pltpu
from jax.sharding import PartitionSpec as P

TILE = 128


VMEM = pl.BlockSpec(memory_space=pltpu.VMEM)
SMEM = pl.BlockSpec(memory_space=pltpu.SMEM)
HBM = pl.BlockSpec(memory_space=pltpu.HBM)
ROOM = pltpu.CompilerParams(vmem_limit_bytes=16 * 2**20)


def spread_rows(tables, parts):
    count, rows, width = tables.shape
    blocks = rows // TILE
    piece = TILE // parts
    shape = (parts, count, blocks, piece, width)

    def kernel(in_ref, out_ref, held, came, left):
        def fetch(table):
            return pltpu.make_async_copy(in_ref.at[table], held.at[table], came.at[table])

        def table_out(table):
            return out_ref.at[:, table]

        for table in range(count):
            fetch(table).start()
        for table in range(count):
            fetch(table).wait()
            for block in range(blocks):
                pltpu.make_async_copy(held.at[table, block], table_out(table).at[:, block], left.at[table]).start()
        for table in range(count):
            pltpu.make_async_copy(table_out(table), table_out(table), left.at[table]).wait()

    return pl.pallas_call(
        kernel,
        in_specs=[HBM],
        out_specs=HBM,
        out_shape=jax.ShapeDtypeStruct(shape, tables.dtype),
        scratch_shapes=[
            pltpu.VMEM((count, blocks, parts, piece, width), tables.dtype),
            pltpu.SemaphoreType.DMA((count,)),
            pltpu.SemaphoreType.DMA((count,)),
        ],
        name="spread_rows",
    )(tables.reshape(count, blocks, parts, piece, width))


def place_pieces(pieces, listing, smalls, owners, total):
    count, piece, width = pieces.shape
    per_owner = total // owners
    chunk = 512
    steps = count // chunk
    batch = 64
    lines = smalls[0].shape[0] - owners

    def kernel(list_ref, in_ref, *refs):
        small_refs = refs[: len(smalls)]
        out_ref, held, places, sums, notes, came, told = refs[len(smalls) :]

        def fetch(step):
            span = pl.ds(step * chunk, chunk)
            return pltpu.make_async_copy(in_ref.at[span], held.at[span], came.at[step])

        telling = pltpu.make_async_copy(list_ref, places, told)
        telling.start()
        for step in range(steps):
            fetch(step).start()
        for at, small_ref in enumerate(small_refs):
            for line in range(lines):
                sums[at * lines + line] = small_ref[line : line + 1]
        notes[...] = sum(small_ref[lines:] for small_ref in small_refs)
        for owner in range(owners):
            out_ref[owner * per_owner + per_owner - 1, 0:1] = notes[owner : owner + 1]
            out_ref[owner * per_owner + per_owner - 1, 1:2] = jnp.zeros((1, width), pieces.dtype)
        telling.wait()
        for owner in range(owners):
            for at in range(piece):
                row = sums[places[count + owner * piece + at]]
                out_ref[owner * per_owner + per_owner - 2, at : at + 1] = row

        def one(step, carry):
            fetch(step).wait()

            def some(at, carry):
                first = step * chunk + at * batch
                rows = [held[first + k] for k in range(batch)]
                for k in range(batch):
                    out_ref[places[first + k]] = rows[k]
                return carry

            return lax.fori_loop(0, chunk // batch, some, carry)

        lax.fori_loop(0, steps, one, 0)

    return pl.pallas_call(
        kernel,
        in_specs=[HBM, HBM] + [VMEM] * len(smalls),
        out_specs=VMEM,
        out_shape=jax.ShapeDtypeStruct((total, piece, width), pieces.dtype),
        scratch_shapes=[
            pltpu.VMEM((count, piece, width), pieces.dtype),
            pltpu.SMEM(listing.shape, jnp.int32),
            pltpu.VMEM((lines * len(smalls), 1, width), pieces.dtype),
            pltpu.VMEM((owners, width), pieces.dtype),
            pltpu.SemaphoreType.DMA((steps,)),
            pltpu.SemaphoreType.DMA,
        ],
        compiler_params=ROOM,
        name="place_pieces",
    )(listing, pieces, *smalls)


def pick_loop(which_ref, in_ref, out_ref, spots, base_of):
    batch = 32

    def one(line, carry):
        base = base_of(line)
        for first in range(0, len(spots), batch):
            rows = [in_ref[which_ref[line, k]] for k in range(first, first + batch)]
            for k in range(batch):
                out_ref[base + spots[first + k]] = rows[k]
        return carry

    lax.fori_loop(0, which_ref.shape[0], one, 0)


def pick_rows(rows, which):
    lines, lanes = which.shape
    width = rows.shape[2]

    def kernel(which_ref, in_ref, out_ref):
        pick_loop(which_ref, in_ref, out_ref, range(lanes), lambda line: line * lanes)

    return pl.pallas_call(
        kernel,
        in_specs=[SMEM, VMEM],
        out_specs=VMEM,
        out_shape=jax.ShapeDtypeStruct((lines * lanes, 1, width), rows.dtype),
        compiler_params=ROOM,
        name="pick_rows",
    )(which, rows)


def answer_and_join(got, which, blocks, spots, base_of):
    parts, _, piece, width = got.shape

    def kernel(which_ref, rows_ref, got_ref, out_ref, table_ref, sums_ref, left):
        for part in range(parts):
            pltpu.make_async_copy(got_ref.at[part, pl.ds(0, blocks)], table_ref.at[:, part], left).start()
        for part in range(parts):
            sums_ref[part] = got_ref[part, blocks]
        pick_loop(which_ref, rows_ref, out_ref, spots, base_of)
        pltpu.make_async_copy(table_ref, table_ref, left).wait()

    return pl.pallas_call(
        kernel,
        in_specs=[SMEM, VMEM, VMEM],
        out_specs=(VMEM, HBM, VMEM),
        out_shape=(
            jax.ShapeDtypeStruct((parts * len(spots), 1, width), got.dtype),
            jax.ShapeDtypeStruct((blocks, parts, piece, width), got.dtype),
            jax.ShapeDtypeStruct((parts, piece, width), got.dtype),
        ),
        scratch_shapes=[pltpu.SemaphoreType.DMA],
        compiler_params=ROOM,
        name="answer_and_join",
    )(which, got.reshape(-1, 1, width), got)


def swap_groups(parts, axis):
    peers = lax.axis_size(axis)
    me = lax.axis_index(axis)
    held = [lax.dynamic_index_in_dim(parts, me, 0, keepdims=False)]
    for by in range(1, peers):
        part = lax.dynamic_index_in_dim(parts, (me + by) % peers, 0, keepdims=False)
        held.append(lax.ppermute(part, axis, [(i, (i + by) % peers) for i in range(peers)]))
    return held


def line_of(group, shard):
    return group // 2 * 128 + shard // 4 % 4 * 32 + shard // 16 * 8 + shard % 4 * 2 + group % 2


def body(tables, accum, block_position, lookup_ids):
    groups = lax.axis_size("grp")
    shards = lax.axis_size("dev")
    my_group = lax.axis_index("grp")
    my_shard = lax.axis_index("dev")
    both = ("grp", "dev")
    table_count, old_rows, width = tables.shape
    per_old = old_rows // TILE
    local = groups * per_old
    piece = TILE // shards
    look_rows = lookup_ids.shape[0]
    limit = 2 * look_rows // shards

    spread = spread_rows(tables, shards)
    spread, accum, block_position, lookup_ids = lax.optimization_barrier(
        (spread, accum, block_position, lookup_ids)
    )
    pieces = lax.all_to_all(
        spread.reshape(shards * groups, per_old, piece, width), ("dev", "grp"), split_axis=0, concat_axis=0, tiled=True
    )

    table_ids = jnp.arange(table_count, dtype=jnp.int32)[None, :]
    id_place = block_position[table_ids, lookup_ids // TILE]
    owner = id_place // local
    per_owner = local + 2
    inside = lookup_ids % TILE
    at_row = (inside // piece * per_owner + id_place % local) * piece + inside % piece
    owner_marks = (owner[..., None] == jnp.arange(shards, dtype=jnp.int32)[None, None, :]).astype(jnp.int32)
    owner_order = jnp.sum((jnp.cumsum(owner_marks, axis=0) - owner_marks) * owner_marks, axis=2)
    table_grid = jnp.broadcast_to(table_ids, owner.shape)
    asking = (
        jnp.zeros((table_count, shards, limit), jnp.int32)
        .at[table_grid, owner, owner_order]
        .set(at_row)
    )

    slot = (line_of(table_grid, owner) * limit + owner_order).reshape(-1, TILE)

    counter = jnp.arange(local, dtype=jnp.int32)
    old_index = (counter // per_old * shards + my_shard) * per_old + counter % per_old
    position_row = lax.dynamic_index_in_dim(block_position, my_group, 0, keepdims=False)
    new_place = position_row[old_index]
    target = new_place // local
    slot_place = new_place % local
    longer = local // 2 + 1
    capacity = -(-longer // shards) + -(-(local - longer) // shards)
    marks = (target[:, None] == jnp.arange(shards, dtype=jnp.int32)[None, :]).astype(jnp.int32)
    order_in = jnp.sum((jnp.cumsum(marks, axis=0) - marks) * marks, axis=1)
    slot_index = target * capacity + order_in
    source_of = jnp.zeros((shards * capacity,), jnp.int32).at[slot_index].set(counter)
    filled = jnp.zeros((shards * capacity,), jnp.int32).at[slot_index].set(1)
    send_place = jnp.where(filled == 1, slot_place[source_of], -1).reshape(shards, capacity)

    asked = groups * limit
    smalls = swap_groups(
        jnp.concatenate(
            [
                accum.reshape(table_count, per_old, TILE),
                lax.dynamic_update_slice(
                    jnp.zeros((table_count, shards, TILE), jnp.float32),
                    asking.astype(jnp.float32),
                    (0, 0, my_group * limit),
                ),
            ],
            axis=1,
        ),
        "grp",
    )
    smalls[0] = smalls[0] + jnp.pad(
        send_place.astype(jnp.float32), ((per_old, 0), (asked, TILE - asked - capacity))
    )
    per_owner = local + 2
    slots = (position_row + position_row // local * 2).reshape(groups, shards, per_old).transpose(1, 0, 2)
    from_small = (my_group - source_of // per_old) % groups * per_old + source_of % per_old
    listing = jnp.concatenate([slots.reshape(-1), from_small])
    pieces, slot = lax.optimization_barrier((pieces, slot))

    sending = place_pieces(
        pieces.reshape(-1, piece, width), listing, smalls, shards, shards * per_owner
    ).reshape(shards, per_owner, piece, width)
    got = lax.all_to_all(sending, "dev", split_axis=0, concat_axis=0, tiled=True)

    got_notes = got[:, local + 1, 0].astype(jnp.int32)
    spots = [line_of(k // limit, 0) * limit + k % limit for k in range(asked)]
    answer, new_table, got_sums = answer_and_join(got, got_notes, local, spots, lambda shard: line_of(0, shard) * limit)
    answer = answer.reshape(groups * shards, limit, width)
    lines = sorted(range(groups * shards), key=lambda device: line_of(device // shards, device % shards))
    returned = lax.all_to_all(answer, both, split_axis=0, concat_axis=0, axis_index_groups=[lines], tiled=True)

    new_table = new_table.reshape(1, local * TILE, width)
    got_sums, late_notes = lax.optimization_barrier((got_sums, got_notes))
    flat_place = late_notes[:, asked : asked + capacity].reshape(-1)
    landing = jnp.where(flat_place >= 0, flat_place, local)
    picker = (
        jnp.zeros((local,), jnp.int32)
        .at[landing]
        .set(jnp.arange(shards * capacity, dtype=jnp.int32), mode="drop")
    )
    new_accum = got_sums.reshape(shards * capacity, TILE)[picker].reshape(1, local * TILE)

    looked = pick_rows(returned.reshape(-1, 1, width), slot)
    looked = looked.reshape(look_rows, table_count, width)
    return (new_table, new_accum, looked)


def solution(mesh):
    placed = (P(None, ("grp", "dev"), None), P(None, ("grp", "dev")), P(), P(("grp", "dev"), None))
    return jax.shard_map(
        body,
        mesh=mesh,
        in_specs=placed,
        out_specs=(P("grp", "dev", None), P("grp", "dev"), P(("grp", "dev"), None, None)),
        check_vma=False,
    )
```

```python
import jax
import jax.numpy as jnp
from jax import lax
from jax.experimental import pallas as pl
from jax.experimental.pallas import tpu as pltpu
from jax.sharding import PartitionSpec as P

TILE = 128


VMEM = pl.BlockSpec(memory_space=pltpu.VMEM)
SMEM = pl.BlockSpec(memory_space=pltpu.SMEM)
HBM = pl.BlockSpec(memory_space=pltpu.HBM)
ROOM = pltpu.CompilerParams(vmem_limit_bytes=16 * 2**20)


def spread_rows(tables, parts):
    count, rows, width = tables.shape
    blocks = rows // TILE
    piece = TILE // parts
    shape = (parts, count, blocks, piece, width)

    def kernel(in_ref, out_ref, held, came, left):
        def fetch(table):
            return pltpu.make_async_copy(in_ref.at[table], held.at[table], came.at[table])

        def table_out(table):
            return out_ref.at[:, table]

        for table in range(count):
            fetch(table).start()
        for table in range(count):
            fetch(table).wait()
            for block in range(blocks):
                pltpu.make_async_copy(held.at[table, block], table_out(table).at[:, block], left.at[table]).start()
        for table in range(count):
            pltpu.make_async_copy(table_out(table), table_out(table), left.at[table]).wait()

    return pl.pallas_call(
        kernel,
        in_specs=[HBM],
        out_specs=HBM,
        out_shape=jax.ShapeDtypeStruct(shape, tables.dtype),
        scratch_shapes=[
            pltpu.VMEM((count, blocks, parts, piece, width), tables.dtype),
            pltpu.SemaphoreType.DMA((count,)),
            pltpu.SemaphoreType.DMA((count,)),
        ],
        name="spread_rows",
    )(tables.reshape(count, blocks, parts, piece, width))


def place_pieces(pieces, listing, smalls, places_row, owners, total):
    count, piece, width = pieces.shape
    groups = len(smalls)
    per_owner = total // owners
    steps = 8
    chunk = count // steps
    batch = 32
    lines = count // owners // groups
    packed = smalls[0].shape[0] - lines
    in_row = owners // packed
    limit = width // in_row

    def kernel(list_ref, in_ref, *refs):
        small_refs = refs[:groups]
        row_ref, out_ref, held, places, sums, notes, came, told = refs[groups:]

        def fetch(step):
            span = pl.ds(step * chunk, chunk)
            return pltpu.make_async_copy(in_ref.at[span], held.at[span], came.at[step])

        telling = pltpu.make_async_copy(list_ref, places, told)
        telling.start()
        for step in range(steps):
            fetch(step).start()
        for at, small_ref in enumerate(small_refs):
            for line in range(lines):
                sums[at * lines + line] = small_ref[line : line + 1]
        telling.wait()
        lane_group = lax.broadcasted_iota(jnp.int32, (packed, width), 1) // limit
        rows = [small_ref[lines:] for small_ref in small_refs]
        senders = [(places[count + owners * piece] + groups - at) & (groups - 1) for at in range(groups)]
        for at in range(in_row):
            mixed = jnp.zeros((packed, width), pieces.dtype)
            for sender, row in zip(senders, rows):
                turn = (sender * limit + width - at * limit) & (width - 1)
                mixed = jnp.where(lane_group == sender, pltpu.roll(row, turn, 1), mixed)
            for line in range(packed):
                notes[line * in_row + at : line * in_row + at + 1] = mixed[line : line + 1]
        notes[...] = notes[...] + row_ref[...]
        for owner in range(owners):
            out_ref[owner * per_owner + per_owner - 1, 0:1] = notes[owner : owner + 1]
            out_ref[owner * per_owner + per_owner - 1, 1:2] = jnp.zeros((1, width), pieces.dtype)
            for at in range(piece):
                row = sums[places[count + owner * piece + at]]
                out_ref[owner * per_owner + per_owner - 2, at : at + 1] = row
        for step in range(steps):
            fetch(step).wait()
            for first in range(step * chunk, (step + 1) * chunk, batch):
                some = [held[k] for k in range(first, first + batch)]
                for k in range(batch):
                    out_ref[places[first + k]] = some[k]

    return pl.pallas_call(
        kernel,
        in_specs=[HBM, HBM] + [VMEM] * (groups + 1),
        out_specs=VMEM,
        out_shape=jax.ShapeDtypeStruct((total, piece, width), pieces.dtype),
        scratch_shapes=[
            pltpu.VMEM((count, piece, width), pieces.dtype),
            pltpu.SMEM(listing.shape, jnp.int32),
            pltpu.VMEM((lines * groups, 1, width), pieces.dtype),
            pltpu.VMEM((owners, width), pieces.dtype),
            pltpu.SemaphoreType.DMA((steps,)),
            pltpu.SemaphoreType.DMA,
        ],
        compiler_params=ROOM,
        name="place_pieces",
    )(listing, pieces, *smalls, places_row)


def pick_all(which_ref, in_ref, out_ref, spot_of):
    lines, _ = which_ref.shape
    for line in range(lines):
        for first in range(0, len(spot_of[line]), 32):
            lanes = range(first, min(first + 32, len(spot_of[line])))
            rows = [in_ref[which_ref[line, k]] for k in lanes]
            for k, row in zip(lanes, rows):
                out_ref[spot_of[line][k]] = row


def pick_rows(rows, which):
    lines, lanes = which.shape
    width = rows.shape[2]

    def kernel(which_ref, in_ref, out_ref):
        pick_all(which_ref, in_ref, out_ref, [range(line * lanes, (line + 1) * lanes) for line in range(lines)])

    return pl.pallas_call(
        kernel,
        in_specs=[SMEM, VMEM],
        out_specs=VMEM,
        out_shape=jax.ShapeDtypeStruct((lines * lanes, 1, width), rows.dtype),
        compiler_params=ROOM,
        name="pick_rows",
    )(which, rows)


def answer_and_join(got, which, blocks, spot_of):
    parts, _, piece, width = got.shape

    def kernel(which_ref, rows_ref, got_ref, out_ref, table_ref, sums_ref, left):
        for part in range(parts):
            pltpu.make_async_copy(got_ref.at[part, pl.ds(0, blocks)], table_ref.at[:, part], left).start()
        for part in range(parts):
            sums_ref[part] = got_ref[part, blocks]
        pick_all(which_ref, rows_ref, out_ref, spot_of)
        pltpu.make_async_copy(table_ref, table_ref, left).wait()

    return pl.pallas_call(
        kernel,
        in_specs=[SMEM, VMEM, VMEM],
        out_specs=(VMEM, HBM, VMEM),
        out_shape=(
            jax.ShapeDtypeStruct((sum(map(len, spot_of)), 1, width), got.dtype),
            jax.ShapeDtypeStruct((blocks, parts, piece, width), got.dtype),
            jax.ShapeDtypeStruct((parts, piece, width), got.dtype),
        ),
        scratch_shapes=[pltpu.SemaphoreType.DMA],
        compiler_params=ROOM,
        name="answer_and_join",
    )(which, got.reshape(-1, 1, width), got)


def swap_groups(parts, axis):
    peers = lax.axis_size(axis)
    me = lax.axis_index(axis)
    held = [lax.dynamic_index_in_dim(parts, me, 0, keepdims=False)]
    for by in range(1, peers):
        part = lax.dynamic_index_in_dim(parts, (me + by) % peers, 0, keepdims=False)
        held.append(lax.ppermute(part, axis, [(i, (i + by) % peers) for i in range(peers)]))
    return held


def line_of(group, shard):
    return group // 2 * 128 + shard // 4 % 4 * 32 + shard // 16 * 8 + shard % 4 * 2 + group % 2


def body(tables, accum, block_position, lookup_ids):
    groups = lax.axis_size("grp")
    shards = lax.axis_size("dev")
    my_group = lax.axis_index("grp")
    my_shard = lax.axis_index("dev")
    both = ("grp", "dev")
    table_count, old_rows, width = tables.shape
    per_old = old_rows // TILE
    local = groups * per_old
    piece = TILE // shards
    look_rows = lookup_ids.shape[0]
    limit = 2 * look_rows // shards

    spread = spread_rows(tables, shards)
    spread, accum, block_position, lookup_ids = lax.optimization_barrier(
        (spread, accum, block_position, lookup_ids)
    )
    pieces = lax.all_to_all(
        spread.reshape(shards * groups, per_old, piece, width), ("dev", "grp"), split_axis=0, concat_axis=0, tiled=True
    )

    table_ids = jnp.arange(table_count, dtype=jnp.int32)[None, :]
    id_place = block_position[table_ids, lookup_ids // TILE]
    owner = id_place // local
    per_owner = local + 2
    inside = lookup_ids % TILE
    at_row = (inside // piece * per_owner + id_place % local) * piece + inside % piece
    owner_marks = (owner[..., None] == jnp.arange(shards, dtype=jnp.int32)[None, None, :]).astype(jnp.int32)
    owner_order = jnp.sum((jnp.cumsum(owner_marks, axis=0) - owner_marks) * owner_marks, axis=2)
    table_grid = jnp.broadcast_to(table_ids, owner.shape)
    asking = (
        jnp.zeros((table_count, shards, limit), jnp.int32)
        .at[table_grid, owner, owner_order]
        .set(at_row)
    )

    slot = (line_of(table_grid, owner) * limit + owner_order).reshape(-1, TILE)

    counter = jnp.arange(local, dtype=jnp.int32)
    old_index = (counter // per_old * shards + my_shard) * per_old + counter % per_old
    position_row = lax.dynamic_index_in_dim(block_position, my_group, 0, keepdims=False)
    new_place = position_row[old_index]
    target = new_place // local
    slot_place = new_place % local
    longer = local // 2 + 1
    capacity = -(-longer // shards) + -(-(local - longer) // shards)
    marks = (target[:, None] == jnp.arange(shards, dtype=jnp.int32)[None, :]).astype(jnp.int32)
    order_in = jnp.sum((jnp.cumsum(marks, axis=0) - marks) * marks, axis=1)
    slot_index = target * capacity + order_in
    source_of = jnp.zeros((shards * capacity,), jnp.int32).at[slot_index].set(counter)
    filled = jnp.zeros((shards * capacity,), jnp.int32).at[slot_index].set(1)
    send_place = jnp.where(filled == 1, slot_place[source_of], -1).reshape(shards, capacity)

    smalls = swap_groups(
        jnp.concatenate(
            [
                accum.reshape(table_count, per_old, TILE),
                asking.astype(jnp.float32).reshape(table_count, -1, TILE),
            ],
            axis=1,
        ),
        "grp",
    )
    asked = groups * limit
    places_row = jnp.pad(send_place.astype(jnp.float32), ((0, 0), (asked, TILE - asked - capacity)))
    per_owner = local + 2
    slots = (position_row + position_row // local * 2).reshape(groups, shards, per_old).transpose(1, 0, 2)
    from_small = (my_group - source_of // per_old) % groups * per_old + source_of % per_old
    listing = jnp.concatenate([slots.reshape(-1), from_small, jnp.full((TILE,), my_group, jnp.int32)])
    pieces, slot = lax.optimization_barrier((pieces, slot))

    sending = place_pieces(
        pieces.reshape(-1, piece, width), listing, smalls, places_row, shards, shards * per_owner
    ).reshape(shards, per_owner, piece, width)
    got = lax.all_to_all(sending, "dev", split_axis=0, concat_axis=0, tiled=True)

    got_notes = got[:, local + 1, 0].astype(jnp.int32)
    spot_of = [
        [line_of(k // limit, shard) * limit + k % limit for k in range(asked)] for shard in range(shards)
    ]
    answer, new_table, got_sums = answer_and_join(got, got_notes, local, spot_of)
    answer = answer.reshape(groups * shards, limit, width)
    lines = sorted(range(groups * shards), key=lambda device: line_of(device // shards, device % shards))
    returned = lax.all_to_all(answer, both, split_axis=0, concat_axis=0, axis_index_groups=[lines], tiled=True)

    new_table = new_table.reshape(1, local * TILE, width)
    got_sums, late_notes = lax.optimization_barrier((got_sums, got_notes))
    flat_place = late_notes[:, asked : asked + capacity].reshape(-1)
    landing = jnp.where(flat_place >= 0, flat_place, local)
    picker = (
        jnp.zeros((local,), jnp.int32)
        .at[landing]
        .set(jnp.arange(shards * capacity, dtype=jnp.int32), mode="drop")
    )
    new_accum = got_sums.reshape(shards * capacity, TILE)[picker].reshape(1, local * TILE)

    looked = pick_rows(returned.reshape(-1, 1, width), slot)
    looked = looked.reshape(look_rows, table_count, width)
    return (new_table, new_accum, looked)


def solution(mesh):
    placed = (P(None, ("grp", "dev"), None), P(None, ("grp", "dev")), P(), P(("grp", "dev"), None))
    return jax.shard_map(
        body,
        mesh=mesh,
        in_specs=placed,
        out_specs=(P("grp", "dev", None), P("grp", "dev"), P(("grp", "dev"), None, None)),
        check_vma=False,
    )
```

```python
import jax
import jax.numpy as jnp
from jax import lax
from jax.experimental import pallas as pl
from jax.experimental.pallas import tpu as pltpu
from jax.sharding import PartitionSpec as P

TILE = 128


VMEM = pl.BlockSpec(memory_space=pltpu.VMEM)
SMEM = pl.BlockSpec(memory_space=pltpu.SMEM)
HBM = pl.BlockSpec(memory_space=pltpu.HBM)
ROOM = pltpu.CompilerParams(vmem_limit_bytes=16 * 2**20)


def spread_rows(tables, parts):
    count, rows, width = tables.shape
    blocks = rows // TILE
    piece = TILE // parts
    shape = (parts, count, blocks, piece, width)

    def kernel(in_ref, out_ref, held, came, left):
        def fetch(table):
            return pltpu.make_async_copy(in_ref.at[table], held.at[table], came.at[table])

        def table_out(table):
            return out_ref.at[:, table]

        for table in range(count):
            fetch(table).start()
        for table in range(count):
            fetch(table).wait()
            for block in range(blocks):
                pltpu.make_async_copy(held.at[table, block], table_out(table).at[:, block], left.at[table]).start()
        for table in range(count):
            pltpu.make_async_copy(table_out(table), table_out(table), left.at[table]).wait()

    return pl.pallas_call(
        kernel,
        in_specs=[HBM],
        out_specs=HBM,
        out_shape=jax.ShapeDtypeStruct(shape, tables.dtype),
        scratch_shapes=[
            pltpu.VMEM((count, blocks, parts, piece, width), tables.dtype),
            pltpu.SemaphoreType.DMA((count,)),
            pltpu.SemaphoreType.DMA((count,)),
        ],
        name="spread_rows",
    )(tables.reshape(count, blocks, parts, piece, width))


def place_pieces(pieces, listing, smalls, places_row, owners, total):
    count, piece, width = pieces.shape
    groups = len(smalls)
    per_owner = total // owners
    steps = 8
    chunk = count // steps
    batch = 32
    lines = count // owners // groups
    packed = smalls[0].shape[0] - lines
    in_row = owners // packed
    limit = width // in_row

    def kernel(list_ref, in_ref, *refs):
        small_refs = refs[:groups]
        row_ref, out_ref, held, places, sums, notes, came, told = refs[groups:]

        def fetch(step):
            span = pl.ds(step * chunk, chunk)
            return pltpu.make_async_copy(in_ref.at[span], held.at[span], came.at[step])

        telling = pltpu.make_async_copy(list_ref, places, told)
        telling.start()
        for step in range(steps):
            fetch(step).start()
        for at, small_ref in enumerate(small_refs):
            for line in range(lines):
                sums[at * lines + line] = small_ref[line : line + 1]
        telling.wait()
        lane_group = lax.broadcasted_iota(jnp.int32, (packed, width), 1) // limit
        rows = [small_ref[lines:] for small_ref in small_refs]
        senders = [(places[count + owners * piece] + groups - at) & (groups - 1) for at in range(groups)]
        for at in range(in_row):
            mixed = jnp.zeros((packed, width), pieces.dtype)
            for sender, row in zip(senders, rows):
                turn = (sender * limit + width - at * limit) & (width - 1)
                mixed = jnp.where(lane_group == sender, pltpu.roll(row, turn, 1), mixed)
            for line in range(packed):
                notes[line * in_row + at : line * in_row + at + 1] = mixed[line : line + 1]
        notes[...] = notes[...] + row_ref[...]
        for owner in range(owners):
            out_ref[owner * per_owner + per_owner - 1, 0:1] = notes[owner : owner + 1]
            out_ref[owner * per_owner + per_owner - 1, 1:2] = jnp.zeros((1, width), pieces.dtype)
            for at in range(piece):
                row = sums[places[count + owner * piece + at]]
                out_ref[owner * per_owner + per_owner - 2, at : at + 1] = row
        for step in range(steps):
            fetch(step).wait()
            for first in range(step * chunk, (step + 1) * chunk, batch):
                some = [held[k] for k in range(first, first + batch)]
                for k in range(batch):
                    out_ref[places[first + k]] = some[k]

    return pl.pallas_call(
        kernel,
        in_specs=[HBM, HBM] + [VMEM] * (groups + 1),
        out_specs=VMEM,
        out_shape=jax.ShapeDtypeStruct((total, piece, width), pieces.dtype),
        scratch_shapes=[
            pltpu.VMEM((count, piece, width), pieces.dtype),
            pltpu.SMEM(listing.shape, jnp.int32),
            pltpu.VMEM((lines * groups, 1, width), pieces.dtype),
            pltpu.VMEM((owners, width), pieces.dtype),
            pltpu.SemaphoreType.DMA((steps,)),
            pltpu.SemaphoreType.DMA,
        ],
        compiler_params=ROOM,
        name="place_pieces",
    )(listing, pieces, *smalls, places_row)


def pick_all(which_ref, in_ref, out_ref, spot_of):
    lines, _ = which_ref.shape
    for line in range(lines):
        for first in range(0, len(spot_of[line]), 32):
            lanes = range(first, min(first + 32, len(spot_of[line])))
            rows = [in_ref[which_ref[line, k]] for k in lanes]
            for k, row in zip(lanes, rows):
                out_ref[spot_of[line][k]] = row


def pick_rows(rows, which):
    lines, lanes = which.shape
    width = rows.shape[2]

    def kernel(which_ref, in_ref, out_ref):
        pick_all(which_ref, in_ref, out_ref, [range(line * lanes, (line + 1) * lanes) for line in range(lines)])

    return pl.pallas_call(
        kernel,
        in_specs=[SMEM, VMEM],
        out_specs=VMEM,
        out_shape=jax.ShapeDtypeStruct((lines * lanes, 1, width), rows.dtype),
        compiler_params=ROOM,
        name="pick_rows",
    )(which, rows)


def answer_and_join(got, which, blocks, spot_of):
    parts, _, piece, width = got.shape
    asked = len(spot_of[0])

    def kernel(list_ref, rows_ref, got_ref, out_ref, table_ref, sums_ref, which_ref, sums, told, left):
        telling = pltpu.make_async_copy(list_ref, which_ref, told)
        telling.start()
        for part in range(parts):
            pltpu.make_async_copy(got_ref.at[part, pl.ds(0, blocks)], table_ref.at[:, part], left).start()
        telling.wait()
        pick_all(which_ref, rows_ref, out_ref, spot_of)
        for part in range(parts):
            for at in range(piece):
                sums[which_ref[part, asked + at]] = got_ref[part, blocks, at : at + 1]
        for block in range(blocks):
            sums_ref[block] = sums[block]
        pltpu.make_async_copy(table_ref, table_ref, left).wait()

    return pl.pallas_call(
        kernel,
        in_specs=[HBM, VMEM, VMEM],
        out_specs=(VMEM, HBM, VMEM),
        out_shape=(
            jax.ShapeDtypeStruct((sum(map(len, spot_of)), 1, width), got.dtype),
            jax.ShapeDtypeStruct((blocks, parts, piece, width), got.dtype),
            jax.ShapeDtypeStruct((blocks, 1, width), got.dtype),
        ),
        scratch_shapes=[
            pltpu.SMEM(which.shape, jnp.int32),
            pltpu.VMEM((blocks + 1, 1, width), got.dtype),
            pltpu.SemaphoreType.DMA,
            pltpu.SemaphoreType.DMA,
        ],
        compiler_params=ROOM,
        name="answer_and_join",
    )(which, got.reshape(-1, 1, width), got)


def swap_groups(parts, axis):
    peers = lax.axis_size(axis)
    me = lax.axis_index(axis)
    held = [lax.dynamic_index_in_dim(parts, me, 0, keepdims=False)]
    for by in range(1, peers):
        part = lax.dynamic_index_in_dim(parts, (me + by) % peers, 0, keepdims=False)
        held.append(lax.ppermute(part, axis, [(i, (i + by) % peers) for i in range(peers)]))
    return held


def line_of(group, shard):
    return group // 2 * 128 + shard // 4 % 4 * 32 + shard // 16 * 8 + shard % 4 * 2 + group % 2


def body(tables, accum, block_position, lookup_ids):
    groups = lax.axis_size("grp")
    shards = lax.axis_size("dev")
    my_group = lax.axis_index("grp")
    my_shard = lax.axis_index("dev")
    both = ("grp", "dev")
    table_count, old_rows, width = tables.shape
    per_old = old_rows // TILE
    local = groups * per_old
    piece = TILE // shards
    look_rows = lookup_ids.shape[0]
    limit = 2 * look_rows // shards

    spread = spread_rows(tables, shards)
    spread, accum, block_position, lookup_ids = lax.optimization_barrier(
        (spread, accum, block_position, lookup_ids)
    )
    pieces = lax.all_to_all(
        spread.reshape(shards * groups, per_old, piece, width), ("dev", "grp"), split_axis=0, concat_axis=0, tiled=True
    )

    table_ids = jnp.arange(table_count, dtype=jnp.int32)[None, :]
    id_place = block_position[table_ids, lookup_ids // TILE]
    owner = id_place // local
    per_owner = local + 2
    inside = lookup_ids % TILE
    at_row = (inside // piece * per_owner + id_place % local) * piece + inside % piece
    owner_marks = (owner[..., None] == jnp.arange(shards, dtype=jnp.int32)[None, None, :]).astype(jnp.int32)
    owner_order = jnp.sum((jnp.cumsum(owner_marks, axis=0) - owner_marks) * owner_marks, axis=2)
    table_grid = jnp.broadcast_to(table_ids, owner.shape)
    asking = (
        jnp.zeros((table_count, shards, limit), jnp.int32)
        .at[table_grid, owner, owner_order]
        .set(at_row)
    )

    slot = (line_of(table_grid, owner) * limit + owner_order).reshape(-1, TILE)

    counter = jnp.arange(local, dtype=jnp.int32)
    old_index = (counter // per_old * shards + my_shard) * per_old + counter % per_old
    position_row = lax.dynamic_index_in_dim(block_position, my_group, 0, keepdims=False)
    new_place = position_row[old_index]
    target = new_place // local
    slot_place = new_place % local
    longer = local // 2 + 1
    capacity = -(-longer // shards) + -(-(local - longer) // shards)
    marks = (target[:, None] == jnp.arange(shards, dtype=jnp.int32)[None, :]).astype(jnp.int32)
    order_in = jnp.sum((jnp.cumsum(marks, axis=0) - marks) * marks, axis=1)
    slot_index = target * capacity + order_in
    source_of = jnp.zeros((shards * capacity,), jnp.int32).at[slot_index].set(counter)
    filled = jnp.zeros((shards * capacity,), jnp.int32).at[slot_index].set(1)
    send_place = jnp.where(filled == 1, slot_place[source_of], local).reshape(shards, capacity)

    smalls = swap_groups(
        jnp.concatenate(
            [
                accum.reshape(table_count, per_old, TILE),
                asking.astype(jnp.float32).reshape(table_count, -1, TILE),
            ],
            axis=1,
        ),
        "grp",
    )
    asked = groups * limit
    places_row = jnp.pad(send_place.astype(jnp.float32), ((0, 0), (asked, TILE - asked - capacity)))
    per_owner = local + 2
    slots = (position_row + position_row // local * 2).reshape(groups, shards, per_old).transpose(1, 0, 2)
    from_small = (my_group - source_of // per_old) % groups * per_old + source_of % per_old
    listing = jnp.concatenate([slots.reshape(-1), from_small, jnp.full((TILE,), my_group, jnp.int32)])
    pieces, slot = lax.optimization_barrier((pieces, slot))

    sending = place_pieces(
        pieces.reshape(-1, piece, width), listing, smalls, places_row, shards, shards * per_owner
    ).reshape(shards, per_owner, piece, width)
    got = lax.all_to_all(sending, "dev", split_axis=0, concat_axis=0, tiled=True)

    got_notes = got[:, local + 1, 0].astype(jnp.int32)
    spot_of = [
        [line_of(k // limit, shard) * limit + k % limit for k in range(asked)] for shard in range(shards)
    ]
    answer, new_table, new_sums = answer_and_join(got, got_notes, local, spot_of)
    answer = answer.reshape(groups * shards, limit, width)
    lines = sorted(range(groups * shards), key=lambda device: line_of(device // shards, device % shards))
    returned = lax.all_to_all(answer, both, split_axis=0, concat_axis=0, axis_index_groups=[lines], tiled=True)

    new_table = new_table.reshape(1, local * TILE, width)
    new_accum = new_sums.reshape(1, local * TILE)

    looked = pick_rows(returned.reshape(-1, 1, width), slot)
    looked = looked.reshape(look_rows, table_count, width)
    return (new_table, new_accum, looked)


def solution(mesh):
    placed = (P(None, ("grp", "dev"), None), P(None, ("grp", "dev")), P(), P(("grp", "dev"), None))
    return jax.shard_map(
        body,
        mesh=mesh,
        in_specs=placed,
        out_specs=(P("grp", "dev", None), P("grp", "dev"), P(("grp", "dev"), None, None)),
        check_vma=False,
    )
```

```python
import jax
import jax.numpy as jnp
from jax import lax
from jax.experimental import pallas as pl
from jax.experimental.pallas import tpu as pltpu
from jax.sharding import PartitionSpec as P

TILE = 128


VMEM = pl.BlockSpec(memory_space=pltpu.VMEM)
SMEM = pl.BlockSpec(memory_space=pltpu.SMEM)
HBM = pl.BlockSpec(memory_space=pltpu.HBM)
ROOM = pltpu.CompilerParams(vmem_limit_bytes=16 * 2**20)


def spread_rows(tables, parts):
    count, rows, width = tables.shape
    blocks = rows // TILE
    piece = TILE // parts
    shape = (parts, count, blocks, piece, width)

    def kernel(in_ref, out_ref, held, came, left):
        def fetch(table):
            return pltpu.make_async_copy(in_ref.at[table], held.at[table], came.at[table])

        def table_out(table):
            return out_ref.at[:, table]

        for table in range(count):
            fetch(table).start()
        for table in range(count):
            fetch(table).wait()
            for block in range(blocks):
                pltpu.make_async_copy(held.at[table, block], table_out(table).at[:, block], left.at[table]).start()
        for table in range(count):
            pltpu.make_async_copy(table_out(table), table_out(table), left.at[table]).wait()

    return pl.pallas_call(
        kernel,
        in_specs=[HBM],
        out_specs=HBM,
        out_shape=jax.ShapeDtypeStruct(shape, tables.dtype),
        scratch_shapes=[
            pltpu.VMEM((count, blocks, parts, piece, width), tables.dtype),
            pltpu.SemaphoreType.DMA((count,)),
            pltpu.SemaphoreType.DMA((count,)),
        ],
        name="spread_rows",
    )(tables.reshape(count, blocks, parts, piece, width))


def place_pieces(pieces, listing, smalls, places_row, owners, total):
    count, piece, width = pieces.shape
    groups = len(smalls)
    per_owner = total // owners
    steps = 8
    chunk = count // steps
    batch = 32
    lines = count // owners // groups
    packed = smalls[0].shape[0] - lines
    in_row = owners // packed
    limit = width // in_row

    def kernel(list_ref, in_ref, *refs):
        small_refs = refs[:groups]
        row_ref, out_ref, held, places, sums, notes, came, told = refs[groups:]

        def fetch(step):
            span = pl.ds(step * chunk, chunk)
            return pltpu.make_async_copy(in_ref.at[span], held.at[span], came.at[step])

        telling = pltpu.make_async_copy(list_ref, places, told)
        telling.start()
        for step in range(steps):
            fetch(step).start()
        for at, small_ref in enumerate(small_refs):
            for line in range(lines):
                sums[at * lines + line] = small_ref[line : line + 1]
        telling.wait()
        lane_group = lax.broadcasted_iota(jnp.int32, (packed, width), 1) // limit
        rows = [small_ref[lines:] for small_ref in small_refs]
        senders = [(places[count + owners * piece] + groups - at) & (groups - 1) for at in range(groups)]
        for at in range(in_row):
            mixed = jnp.zeros((packed, width), pieces.dtype)
            for sender, row in zip(senders, rows):
                turn = (sender * limit + width - at * limit) & (width - 1)
                mixed = jnp.where(lane_group == sender, pltpu.roll(row, turn, 1), mixed)
            for line in range(packed):
                notes[line * in_row + at : line * in_row + at + 1] = mixed[line : line + 1]
        notes[...] = notes[...] + row_ref[...]
        for owner in range(owners):
            out_ref[owner * per_owner + per_owner - 1, 0:1] = notes[owner : owner + 1]
            out_ref[owner * per_owner + per_owner - 1, 1:2] = jnp.zeros((1, width), pieces.dtype)
            for at in range(piece):
                row = sums[places[count + owner * piece + at]]
                out_ref[owner * per_owner + per_owner - 2, at : at + 1] = row
        for step in range(steps):
            fetch(step).wait()
            for first in range(step * chunk, (step + 1) * chunk, batch):
                some = [held[k] for k in range(first, first + batch)]
                for k in range(batch):
                    out_ref[places[first + k]] = some[k]

    return pl.pallas_call(
        kernel,
        in_specs=[HBM, HBM] + [VMEM] * (groups + 1),
        out_specs=VMEM,
        out_shape=jax.ShapeDtypeStruct((total, piece, width), pieces.dtype),
        scratch_shapes=[
            pltpu.VMEM((count, piece, width), pieces.dtype),
            pltpu.SMEM(listing.shape, jnp.int32),
            pltpu.VMEM((lines * groups, 1, width), pieces.dtype),
            pltpu.VMEM((owners, width), pieces.dtype),
            pltpu.SemaphoreType.DMA((steps,)),
            pltpu.SemaphoreType.DMA,
        ],
        compiler_params=ROOM,
        name="place_pieces",
    )(listing, pieces, *smalls, places_row)


def pick_all(which_ref, in_ref, out_ref, spot_of):
    lines, _ = which_ref.shape
    for line in range(lines):
        for first in range(0, len(spot_of[line]), 32):
            lanes = range(first, min(first + 32, len(spot_of[line])))
            rows = [in_ref[which_ref[line, k]] for k in lanes]
            for k, row in zip(lanes, rows):
                out_ref[spot_of[line][k]] = row


def join_some(got_ref, table_ref, parts, left):
    blocks = table_ref.shape[0]
    for part in parts:
        pltpu.make_async_copy(got_ref.at[part, pl.ds(0, blocks)], table_ref.at[:, part], left).start()
    some = table_ref.at[:, pl.ds(parts[0], len(parts))]
    return pltpu.make_async_copy(some, some, left)


def look_and_join(returned, which, got, table, done):
    lines, lanes = which.shape
    width = returned.shape[2]
    parts = got.shape[0]

    def kernel(list_ref, rows_ref, got_ref, _, out_ref, table_ref, which_ref, told, left):
        telling = pltpu.make_async_copy(list_ref, which_ref, told)
        telling.start()
        joining = join_some(got_ref, table_ref, range(done, parts), left)
        telling.wait()
        pick_all(which_ref, rows_ref, out_ref, [range(line * lanes, (line + 1) * lanes) for line in range(lines)])
        joining.wait()

    return pl.pallas_call(
        kernel,
        in_specs=[HBM, VMEM, VMEM, HBM],
        out_specs=(VMEM, HBM),
        out_shape=(
            jax.ShapeDtypeStruct((lines * lanes, 1, width), returned.dtype),
            jax.ShapeDtypeStruct(table.shape, table.dtype),
        ),
        input_output_aliases={3: 1},
        scratch_shapes=[pltpu.SMEM(which.shape, jnp.int32), pltpu.SemaphoreType.DMA, pltpu.SemaphoreType.DMA],
        compiler_params=ROOM,
        name="look_and_join",
    )(which, returned, got, table)


def answer_and_join(got, which, blocks, spot_of, done):
    parts, _, piece, width = got.shape
    asked = len(spot_of[0])

    def kernel(list_ref, rows_ref, got_ref, out_ref, table_ref, sums_ref, which_ref, sums, told, left):
        telling = pltpu.make_async_copy(list_ref, which_ref, told)
        telling.start()
        joining = join_some(got_ref, table_ref, range(done), left)
        telling.wait()
        pick_all(which_ref, rows_ref, out_ref, spot_of)
        for part in range(parts):
            for at in range(piece):
                sums[which_ref[part, asked + at]] = got_ref[part, blocks, at : at + 1]
        for block in range(blocks):
            sums_ref[block] = sums[block]
        joining.wait()

    return pl.pallas_call(
        kernel,
        in_specs=[HBM, VMEM, VMEM],
        out_specs=(VMEM, HBM, VMEM),
        out_shape=(
            jax.ShapeDtypeStruct((sum(map(len, spot_of)), 1, width), got.dtype),
            jax.ShapeDtypeStruct((blocks, parts, piece, width), got.dtype),
            jax.ShapeDtypeStruct((blocks, 1, width), got.dtype),
        ),
        scratch_shapes=[
            pltpu.SMEM(which.shape, jnp.int32),
            pltpu.VMEM((blocks + 1, 1, width), got.dtype),
            pltpu.SemaphoreType.DMA,
            pltpu.SemaphoreType.DMA,
        ],
        compiler_params=ROOM,
        name="answer_and_join",
    )(which, got.reshape(-1, 1, width), got)


def swap_groups(parts, axis):
    peers = lax.axis_size(axis)
    me = lax.axis_index(axis)
    held = [lax.dynamic_index_in_dim(parts, me, 0, keepdims=False)]
    for by in range(1, peers):
        part = lax.dynamic_index_in_dim(parts, (me + by) % peers, 0, keepdims=False)
        held.append(lax.ppermute(part, axis, [(i, (i + by) % peers) for i in range(peers)]))
    return held


def line_of(group, shard):
    return group // 2 * 128 + shard // 4 % 4 * 32 + shard // 16 * 8 + shard % 4 * 2 + group % 2


def body(tables, accum, block_position, lookup_ids):
    groups = lax.axis_size("grp")
    shards = lax.axis_size("dev")
    my_group = lax.axis_index("grp")
    my_shard = lax.axis_index("dev")
    both = ("grp", "dev")
    table_count, old_rows, width = tables.shape
    per_old = old_rows // TILE
    local = groups * per_old
    piece = TILE // shards
    look_rows = lookup_ids.shape[0]
    limit = 2 * look_rows // shards

    spread = spread_rows(tables, shards)
    spread, accum, block_position, lookup_ids = lax.optimization_barrier(
        (spread, accum, block_position, lookup_ids)
    )
    pieces = lax.all_to_all(
        spread.reshape(shards * groups, per_old, piece, width), ("dev", "grp"), split_axis=0, concat_axis=0, tiled=True
    )

    table_ids = jnp.arange(table_count, dtype=jnp.int32)[None, :]
    id_place = block_position[table_ids, lookup_ids // TILE]
    owner = id_place // local
    per_owner = local + 2
    inside = lookup_ids % TILE
    at_row = (inside // piece * per_owner + id_place % local) * piece + inside % piece
    owner_marks = (owner[..., None] == jnp.arange(shards, dtype=jnp.int32)[None, None, :]).astype(jnp.int32)
    owner_order = jnp.sum((jnp.cumsum(owner_marks, axis=0) - owner_marks) * owner_marks, axis=2)
    table_grid = jnp.broadcast_to(table_ids, owner.shape)
    asking = (
        jnp.zeros((table_count, shards, limit), jnp.int32)
        .at[table_grid, owner, owner_order]
        .set(at_row)
    )

    slot = (line_of(table_grid, owner) * limit + owner_order).reshape(-1, TILE)

    counter = jnp.arange(local, dtype=jnp.int32)
    old_index = (counter // per_old * shards + my_shard) * per_old + counter % per_old
    position_row = lax.dynamic_index_in_dim(block_position, my_group, 0, keepdims=False)
    new_place = position_row[old_index]
    target = new_place // local
    slot_place = new_place % local
    longer = local // 2 + 1
    capacity = -(-longer // shards) + -(-(local - longer) // shards)
    marks = (target[:, None] == jnp.arange(shards, dtype=jnp.int32)[None, :]).astype(jnp.int32)
    order_in = jnp.sum((jnp.cumsum(marks, axis=0) - marks) * marks, axis=1)
    slot_index = target * capacity + order_in
    source_of = jnp.zeros((shards * capacity,), jnp.int32).at[slot_index].set(counter)
    filled = jnp.zeros((shards * capacity,), jnp.int32).at[slot_index].set(1)
    send_place = jnp.where(filled == 1, slot_place[source_of], local).reshape(shards, capacity)

    smalls = swap_groups(
        jnp.concatenate(
            [
                accum.reshape(table_count, per_old, TILE),
                asking.astype(jnp.float32).reshape(table_count, -1, TILE),
            ],
            axis=1,
        ),
        "grp",
    )
    asked = groups * limit
    places_row = jnp.pad(send_place.astype(jnp.float32), ((0, 0), (asked, TILE - asked - capacity)))
    per_owner = local + 2
    slots = (position_row + position_row // local * 2).reshape(groups, shards, per_old).transpose(1, 0, 2)
    from_small = (my_group - source_of // per_old) % groups * per_old + source_of % per_old
    listing = jnp.concatenate([slots.reshape(-1), from_small, jnp.full((TILE,), my_group, jnp.int32)])
    pieces, slot = lax.optimization_barrier((pieces, slot))

    sending = place_pieces(
        pieces.reshape(-1, piece, width), listing, smalls, places_row, shards, shards * per_owner
    ).reshape(shards, per_owner, piece, width)
    got = lax.all_to_all(sending, "dev", split_axis=0, concat_axis=0, tiled=True)

    got_notes = got[:, local + 1, 0].astype(jnp.int32)
    spot_of = [
        [line_of(k // limit, shard) * limit + k % limit for k in range(asked)] for shard in range(shards)
    ]
    joined = shards * 5 // 8
    answer, new_table, new_sums = answer_and_join(got, got_notes, local, spot_of, joined)
    answer = answer.reshape(groups * shards, limit, width)
    lines = sorted(range(groups * shards), key=lambda device: line_of(device // shards, device % shards))
    returned = lax.all_to_all(answer, both, split_axis=0, concat_axis=0, axis_index_groups=[lines], tiled=True)

    looked, new_table = look_and_join(returned.reshape(-1, 1, width), slot, got, new_table, joined)
    looked = looked.reshape(look_rows, table_count, width)
    new_table = new_table.reshape(1, local * TILE, width)
    new_accum = new_sums.reshape(1, local * TILE)
    return (new_table, new_accum, looked)


def solution(mesh):
    placed = (P(None, ("grp", "dev"), None), P(None, ("grp", "dev")), P(), P(("grp", "dev"), None))
    return jax.shard_map(
        body,
        mesh=mesh,
        in_specs=placed,
        out_specs=(P("grp", "dev", None), P("grp", "dev"), P(("grp", "dev"), None, None)),
        check_vma=False,
    )
```

```python
import jax
import jax.numpy as jnp
from jax import lax
from jax.experimental import pallas as pl
from jax.experimental.pallas import tpu as pltpu
from jax.sharding import PartitionSpec as P

TILE = 128


VMEM = pl.BlockSpec(memory_space=pltpu.VMEM)
SMEM = pl.BlockSpec(memory_space=pltpu.SMEM)
HBM = pl.BlockSpec(memory_space=pltpu.HBM)
ROOM = pltpu.CompilerParams(vmem_limit_bytes=16 * 2**20)


def spread_rows(tables, parts):
    count, rows, width = tables.shape
    blocks = rows // TILE
    piece = TILE // parts
    shape = (parts, count, blocks, piece, width)

    cuts = 4
    span = blocks // cuts

    def kernel(in_ref, out_ref, held, came, left):
        def fetch(table, cut):
            some = pl.ds(cut * span, span)
            return pltpu.make_async_copy(in_ref.at[table, some], held.at[table, some], came.at[table, cut])

        def table_out(table):
            return out_ref.at[:, table]

        for table in range(count):
            for cut in range(cuts):
                fetch(table, cut).start()
        for table in range(count):
            for cut in range(cuts):
                fetch(table, cut).wait()
                for block in range(cut * span, (cut + 1) * span):
                    pltpu.make_async_copy(held.at[table, block], table_out(table).at[:, block], left.at[table]).start()
        for table in range(count):
            pltpu.make_async_copy(table_out(table), table_out(table), left.at[table]).wait()

    return pl.pallas_call(
        kernel,
        in_specs=[HBM],
        out_specs=HBM,
        out_shape=jax.ShapeDtypeStruct(shape, tables.dtype),
        scratch_shapes=[
            pltpu.VMEM((count, blocks, parts, piece, width), tables.dtype),
            pltpu.SemaphoreType.DMA((count, cuts)),
            pltpu.SemaphoreType.DMA((count,)),
        ],
        name="spread_rows",
    )(tables.reshape(count, blocks, parts, piece, width))


def place_pieces(pieces, listing, smalls, places_row, owners, total):
    count, piece, width = pieces.shape
    groups = len(smalls)
    per_owner = total // owners
    steps = 8
    chunk = count // steps
    batch = 32
    lines = count // owners // groups
    packed = smalls[0].shape[0] - lines
    in_row = owners // packed
    limit = width // in_row

    def kernel(list_ref, in_ref, *refs):
        small_refs = refs[:groups]
        row_ref, out_ref, held, places, sums, notes, came, told = refs[groups:]

        def fetch(step):
            span = pl.ds(step * chunk, chunk)
            return pltpu.make_async_copy(in_ref.at[span], held.at[span], came.at[step])

        telling = pltpu.make_async_copy(list_ref, places, told)
        telling.start()
        for step in range(steps):
            fetch(step).start()
        for at, small_ref in enumerate(small_refs):
            for line in range(lines):
                sums[at * lines + line] = small_ref[line : line + 1]
        telling.wait()
        lane_group = lax.broadcasted_iota(jnp.int32, (packed, width), 1) // limit
        rows = [small_ref[lines:] for small_ref in small_refs]
        senders = [(places[count + owners * piece] + groups - at) & (groups - 1) for at in range(groups)]
        for at in range(in_row):
            mixed = jnp.zeros((packed, width), pieces.dtype)
            for sender, row in zip(senders, rows):
                turn = (sender * limit + width - at * limit) & (width - 1)
                mixed = jnp.where(lane_group == sender, pltpu.roll(row, turn, 1), mixed)
            for line in range(packed):
                notes[line * in_row + at : line * in_row + at + 1] = mixed[line : line + 1]
        notes[...] = notes[...] + row_ref[...]
        for owner in range(owners):
            out_ref[owner * per_owner + per_owner - 1, 0:1] = notes[owner : owner + 1]
            out_ref[owner * per_owner + per_owner - 1, 1:2] = jnp.zeros((1, width), pieces.dtype)
            for at in range(piece):
                row = sums[places[count + owner * piece + at]]
                out_ref[owner * per_owner + per_owner - 2, at : at + 1] = row
        for step in range(steps):
            fetch(step).wait()
            for first in range(step * chunk, (step + 1) * chunk, batch):
                some = [held[k] for k in range(first, first + batch)]
                for k in range(batch):
                    out_ref[places[first + k]] = some[k]

    return pl.pallas_call(
        kernel,
        in_specs=[HBM, HBM] + [VMEM] * (groups + 1),
        out_specs=VMEM,
        out_shape=jax.ShapeDtypeStruct((total, piece, width), pieces.dtype),
        scratch_shapes=[
            pltpu.VMEM((count, piece, width), pieces.dtype),
            pltpu.SMEM(listing.shape, jnp.int32),
            pltpu.VMEM((lines * groups, 1, width), pieces.dtype),
            pltpu.VMEM((owners, width), pieces.dtype),
            pltpu.SemaphoreType.DMA((steps,)),
            pltpu.SemaphoreType.DMA,
        ],
        compiler_params=ROOM,
        name="place_pieces",
    )(listing, pieces, *smalls, places_row)


def pick_all(which_ref, in_ref, out_ref, spot_of):
    lines, _ = which_ref.shape
    for line in range(lines):
        for first in range(0, len(spot_of[line]), 32):
            lanes = range(first, min(first + 32, len(spot_of[line])))
            rows = [in_ref[which_ref[line, k]] for k in lanes]
            for k, row in zip(lanes, rows):
                out_ref[spot_of[line][k]] = row


def pick_rows(rows, which):
    lines, lanes = which.shape
    width = rows.shape[2]

    def kernel(which_ref, in_ref, out_ref):
        pick_all(which_ref, in_ref, out_ref, [range(line * lanes, (line + 1) * lanes) for line in range(lines)])

    return pl.pallas_call(
        kernel,
        in_specs=[SMEM, VMEM],
        out_specs=VMEM,
        out_shape=jax.ShapeDtypeStruct((lines * lanes, 1, width), rows.dtype),
        compiler_params=ROOM,
        name="pick_rows",
    )(which, rows)


def answer_and_join(got, which, blocks, spot_of):
    parts, _, piece, width = got.shape
    asked = len(spot_of[0])

    def kernel(list_ref, rows_ref, got_ref, out_ref, table_ref, sums_ref, which_ref, sums, told, left):
        telling = pltpu.make_async_copy(list_ref, which_ref, told)
        telling.start()
        for part in range(parts):
            pltpu.make_async_copy(got_ref.at[part, pl.ds(0, blocks)], table_ref.at[:, part], left).start()
        telling.wait()
        pick_all(which_ref, rows_ref, out_ref, spot_of)
        for part in range(parts):
            for at in range(piece):
                sums[which_ref[part, asked + at]] = got_ref[part, blocks, at : at + 1]
        for block in range(blocks):
            sums_ref[block] = sums[block]
        pltpu.make_async_copy(table_ref, table_ref, left).wait()

    return pl.pallas_call(
        kernel,
        in_specs=[HBM, VMEM, VMEM],
        out_specs=(VMEM, HBM, VMEM),
        out_shape=(
            jax.ShapeDtypeStruct((sum(map(len, spot_of)), 1, width), got.dtype),
            jax.ShapeDtypeStruct((blocks, parts, piece, width), got.dtype),
            jax.ShapeDtypeStruct((blocks, 1, width), got.dtype),
        ),
        scratch_shapes=[
            pltpu.SMEM(which.shape, jnp.int32),
            pltpu.VMEM((blocks + 1, 1, width), got.dtype),
            pltpu.SemaphoreType.DMA,
            pltpu.SemaphoreType.DMA,
        ],
        compiler_params=ROOM,
        name="answer_and_join",
    )(which, got.reshape(-1, 1, width), got)


def swap_groups(parts, axis):
    peers = lax.axis_size(axis)
    me = lax.axis_index(axis)
    held = [lax.dynamic_index_in_dim(parts, me, 0, keepdims=False)]
    for by in range(1, peers):
        part = lax.dynamic_index_in_dim(parts, (me + by) % peers, 0, keepdims=False)
        held.append(lax.ppermute(part, axis, [(i, (i + by) % peers) for i in range(peers)]))
    return held


def line_of(group, shard):
    return group // 2 * 128 + shard // 4 % 4 * 32 + shard // 16 * 8 + shard % 4 * 2 + group % 2


def body(tables, accum, block_position, lookup_ids):
    groups = lax.axis_size("grp")
    shards = lax.axis_size("dev")
    my_group = lax.axis_index("grp")
    my_shard = lax.axis_index("dev")
    both = ("grp", "dev")
    table_count, old_rows, width = tables.shape
    per_old = old_rows // TILE
    local = groups * per_old
    piece = TILE // shards
    look_rows = lookup_ids.shape[0]
    limit = 2 * look_rows // shards

    spread = spread_rows(tables, shards)
    spread, accum, block_position, lookup_ids = lax.optimization_barrier(
        (spread, accum, block_position, lookup_ids)
    )
    pieces = lax.all_to_all(
        spread.reshape(shards * groups, per_old, piece, width), ("dev", "grp"), split_axis=0, concat_axis=0, tiled=True
    )

    table_ids = jnp.arange(table_count, dtype=jnp.int32)[None, :]
    id_place = block_position[table_ids, lookup_ids // TILE]
    owner = id_place // local
    per_owner = local + 2
    inside = lookup_ids % TILE
    at_row = (inside // piece * per_owner + id_place % local) * piece + inside % piece
    owner_marks = (owner[..., None] == jnp.arange(shards, dtype=jnp.int32)[None, None, :]).astype(jnp.int32)
    owner_order = jnp.sum((jnp.cumsum(owner_marks, axis=0) - owner_marks) * owner_marks, axis=2)
    table_grid = jnp.broadcast_to(table_ids, owner.shape)
    asking = (
        jnp.zeros((table_count, shards, limit), jnp.int32)
        .at[table_grid, owner, owner_order]
        .set(at_row)
    )

    slot = (line_of(table_grid, owner) * limit + owner_order).reshape(-1, TILE)

    counter = jnp.arange(local, dtype=jnp.int32)
    old_index = (counter // per_old * shards + my_shard) * per_old + counter % per_old
    position_row = lax.dynamic_index_in_dim(block_position, my_group, 0, keepdims=False)
    new_place = position_row[old_index]
    target = new_place // local
    slot_place = new_place % local
    longer = local // 2 + 1
    capacity = -(-longer // shards) + -(-(local - longer) // shards)
    marks = (target[:, None] == jnp.arange(shards, dtype=jnp.int32)[None, :]).astype(jnp.int32)
    order_in = jnp.sum((jnp.cumsum(marks, axis=0) - marks) * marks, axis=1)
    slot_index = target * capacity + order_in
    source_of = jnp.zeros((shards * capacity,), jnp.int32).at[slot_index].set(counter)
    filled = jnp.zeros((shards * capacity,), jnp.int32).at[slot_index].set(1)
    send_place = jnp.where(filled == 1, slot_place[source_of], local).reshape(shards, capacity)

    smalls = swap_groups(
        jnp.concatenate(
            [
                accum.reshape(table_count, per_old, TILE),
                asking.astype(jnp.float32).reshape(table_count, -1, TILE),
            ],
            axis=1,
        ),
        "grp",
    )
    asked = groups * limit
    places_row = jnp.pad(send_place.astype(jnp.float32), ((0, 0), (asked, TILE - asked - capacity)))
    per_owner = local + 2
    slots = (position_row + position_row // local * 2).reshape(groups, shards, per_old).transpose(1, 0, 2)
    from_small = (my_group - source_of // per_old) % groups * per_old + source_of % per_old
    listing = jnp.concatenate([slots.reshape(-1), from_small, jnp.full((TILE,), my_group, jnp.int32)])
    pieces, slot = lax.optimization_barrier((pieces, slot))

    sending = place_pieces(
        pieces.reshape(-1, piece, width), listing, smalls, places_row, shards, shards * per_owner
    ).reshape(shards, per_owner, piece, width)
    got = lax.all_to_all(sending, "dev", split_axis=0, concat_axis=0, tiled=True)

    got_notes = got[:, local + 1, 0].astype(jnp.int32)
    spot_of = [
        [line_of(k // limit, shard) * limit + k % limit for k in range(asked)] for shard in range(shards)
    ]
    answer, new_table, new_sums = answer_and_join(got, got_notes, local, spot_of)
    answer = answer.reshape(groups * shards, limit, width)
    lines = sorted(range(groups * shards), key=lambda device: line_of(device // shards, device % shards))
    returned = lax.all_to_all(answer, both, split_axis=0, concat_axis=0, axis_index_groups=[lines], tiled=True)

    new_table = new_table.reshape(1, local * TILE, width)
    new_accum = new_sums.reshape(1, local * TILE)

    looked = pick_rows(returned.reshape(-1, 1, width), slot)
    looked = looked.reshape(look_rows, table_count, width)
    return (new_table, new_accum, looked)


def solution(mesh):
    placed = (P(None, ("grp", "dev"), None), P(None, ("grp", "dev")), P(), P(("grp", "dev"), None))
    return jax.shard_map(
        body,
        mesh=mesh,
        in_specs=placed,
        out_specs=(P("grp", "dev", None), P("grp", "dev"), P(("grp", "dev"), None, None)),
        check_vma=False,
    )
```
